32 devices in a mesh: member: 4 (over z), py: 4 (over x, core), pz: 2 (over y).
Axes of the slice: x: 2, y: 2, z: 4, core: 2. Of those that a mesh axis runs over, the one named last changes fastest.
Arguments:
- velocity_hat: float32 [8, 3, 96, 36864], P('member', None, None, ('py', 'pz')), parts along dimension 0, may hold values from -448 to 448
- time_step: float32 [4], P('member'), parts along dimension 0, may hold values from 0.003 to 0.006
- power: float32 [4], P('member'), parts along dimension 0, may hold values from 20 to 80
- cutoffs: int32 [12], P('member'), parts along dimension 0, may hold values from 48 to 64, as said below
Outputs:
- velocity_next: float32 [8, 3, 96, 36864], P('member', None, None, ('py', 'pz')), parts along dimension 0
- cfl_number: float32 [4], P('member'), parts along dimension 0
- energy: float32 [4], P('member'), parts along dimension 0
The draws below stay inside these ranges and needn't reach their ends.
There are 4 independent parts, one for each index of `member`. The reference program is written for one: setup_inputs(seed, part) draws one part's arguments, and reference() takes and returns one part's arrays. A program takes and returns all parts, laid end to end along the dimension named above; each array names one. Nothing has to cross between parts.
Inputs may be any that keep to these rules, and one draw needn't show every extreme that they name: `cutoffs`: in every draw one of the three equals 64.
All inputs are finite; a program needn't handle non-finite values.
Results may differ from the reference program's by a relative error of at most 0.0002.
Values sent between devices are 32-bit elements; how exact they have to be, the bound alone decides.
A program may use at most 256 MiB of HBM per device.

```python
import math
import jax
import jax.numpy as jnp
from jax import lax

GRID = 192
SECTIONS = 1


def signed_wave(points):
    index = jnp.arange(points, dtype=jnp.int32)
    return jnp.where(index < points // 2, index, index - points)


def draw_velocity_hat(key, part):
    folded = jax.random.fold_in(key, 17)
    noise_key, scale_key = jax.random.split(folded)
    array_shape = (2, 3, GRID // 2, GRID, GRID)
    depth_wave = jnp.arange(GRID // 2, dtype=jnp.int32)[:, None, None]
    across_y = signed_wave(GRID)[None, :, None]
    along_x = signed_wave(GRID)[None, None, :]
    lowest = (depth_wave <= 2) & (jnp.abs(across_y) <= 2) & (jnp.abs(along_x) <= 2)
    values = jnp.clip(jax.random.normal(noise_key, array_shape, jnp.float32), -4.0, 4.0)
    amplify = 64.0
    result = jnp.where(lowest, amplify * values, values).astype(jnp.float32)
    return result.reshape(2, 3, GRID // 2, GRID * GRID)


def draw_cutoffs(key, part):
    folded = jax.random.fold_in(key, 23)
    value_key, pick_key = jax.random.split(folded)
    values = jax.random.randint(value_key, (3,), GRID // 4, GRID // 3 + 1, dtype=jnp.int32)
    chosen = jax.random.randint(pick_key, (), 0, 3, dtype=jnp.int32)
    return jnp.where(jnp.arange(3, dtype=jnp.int32) == chosen, GRID // 3, values).astype(jnp.int32)


def setup_inputs(seed: int = 0, part: int = 0) -> dict:
    key_list = jax.random.split(jax.random.key(seed), 5)
    part_splits = jax.random.split(jax.random.fold_in(key_list[4], part), 5)
    return {
        "velocity_hat": draw_velocity_hat(jax.random.fold_in(jax.random.fold_in(key_list[4], part), 71), part),
        "time_step": jnp.clip(jax.random.uniform(part_splits[1], (1,), jnp.float32, 0.003, 0.006), 0.003, 0.006),
        "power": jnp.clip(jnp.exp(jax.random.uniform(part_splits[2], (1,), jnp.float32, math.log(20.0), math.log(80.0))), 20.0, 80.0),
        "cutoffs": draw_cutoffs(jax.random.fold_in(jax.random.fold_in(key_list[4], part), 71), part),
    }


viscosity = 0.004
keep_share = (0.0, 0.75, 1.0 / 3.0)


def signed_index(points):
    index = jnp.arange(points, dtype=jnp.int32)
    return jnp.where(index < points // 2, index, index - points)


def to_grid(spectra):
    points = spectra.shape[-1]
    result = []
    for component in range(spectra.shape[0]):
        strips = jnp.fft.ifft(jnp.fft.ifft(spectra[component], axis=2), axis=1)
        padded = jnp.concatenate([strips, jnp.zeros_like(strips[:1])], axis=0)
        result.append(jnp.fft.irfft(padded, n=points, axis=0) * (float(points) ** 1.5))
    return jnp.stack(result)


def to_spectrum(fields):
    points = fields.shape[-1]
    result = []
    for component in range(fields.shape[0]):
        planes = jnp.fft.rfft(fields[component], axis=0)[: points // 2]
        result.append(jnp.fft.fft(jnp.fft.fft(planes, axis=1), axis=2) * (float(points) ** -1.5))
    return result


def reference(velocity_hat, time_step, power, cutoffs):
    points = 2 * velocity_hat.shape[2]
    velocity_hat = velocity_hat.reshape(2, 3, points // 2, points, points)
    wave_z = jnp.arange(points // 2, dtype=jnp.int32)[:, None, None]
    wave_y = signed_index(points)[None, :, None]
    wave_x = signed_index(points)[None, None, :]
    keep_mask = ((jnp.abs(wave_x) <= cutoffs[0]) & (jnp.abs(wave_y) <= cutoffs[1]) & (wave_z <= cutoffs[2])).astype(jnp.float32)
    waves = (wave_x.astype(jnp.float32), wave_y.astype(jnp.float32), wave_z.astype(jnp.float32))
    wave_square = waves[0] * waves[0] + waves[1] * waves[1] + waves[2] * waves[2]
    inverse_square = 1.0 / jnp.maximum(wave_square, 1.0)

    def project(field):
        normal_part = waves[0] * field[0] + waves[1] * field[1] + waves[2] * field[2]
        return [keep_mask * (field[axis_index] - waves[axis_index] * normal_part * inverse_square) for axis_index in range(3)]

    step_size = time_step[0]
    current = [lax.complex(velocity_hat[0, axis_index], velocity_hat[1, axis_index]) for axis_index in range(3)]
    initial = current
    cfl_values = []
    energy_values = []
    for section_index in range(SECTIONS):
        solenoidal = project(current)
        if section_index == 0:
            initial = solenoidal
        curled = [waves[1] * solenoidal[2] - waves[2] * solenoidal[1],
                  waves[2] * solenoidal[0] - waves[0] * solenoidal[2],
                  waves[0] * solenoidal[1] - waves[1] * solenoidal[0]]
        vorticity_hat = [1j * term for term in curled]
        physical = to_grid(jnp.stack(solenoidal + vorticity_hat))
        velocity = physical[:3]
        vorticity = physical[3:]
        nonlinear = jnp.stack([velocity[1] * vorticity[2] - velocity[2] * vorticity[1],
                               velocity[2] * vorticity[0] - velocity[0] * vorticity[2],
                               velocity[0] * vorticity[1] - velocity[1] * vorticity[0]])
        fastest = jnp.max(jnp.abs(velocity[0]) + jnp.abs(velocity[1]) + jnp.abs(velocity[2]))
        energy = 0.5 * jnp.sum(velocity * velocity) / float(points ** 3)
        forced = project(to_spectrum(nonlinear))
        forcing = power[0] / jnp.maximum(2.0 * energy, 0.5)
        update = [solenoidal[axis_index] + step_size * (forced[axis_index] + forcing * solenoidal[axis_index] - viscosity * wave_square * solenoidal[axis_index]) for axis_index in range(3)]
        keep_weight = keep_share[section_index]
        current = [keep_weight * initial[axis_index] + (1.0 - keep_weight) * update[axis_index] for axis_index in range(3)]
        cfl_values.append(step_size * fastest * points / (2.0 * math.pi))
        energy_values.append(energy)
    velocity_next = jnp.stack([jnp.stack([jnp.real(term) for term in current]), jnp.stack([jnp.imag(term) for term in current])]).astype(jnp.float32)
    velocity_next = velocity_next.reshape(2, 3, points // 2, points * points)
    return velocity_next, jnp.stack(cfl_values), jnp.stack(energy_values)
```

```python
import math

import jax
import jax.numpy as jnp
from jax import lax
from jax.sharding import PartitionSpec as P

viscosity = 0.004
keep_share = (0.0, 0.75, 1.0 / 3.0)
highest = lax.Precision.HIGH


def phases(length, row_count, col_count, handed):
    row_index = lax.broadcasted_iota(jnp.int32, (row_count, col_count), 0)
    col_index = lax.broadcasted_iota(jnp.int32, (row_count, col_count), 1)
    windings = row_index * col_index % length
    angles = windings.astype(jnp.float32) * (2.0 * math.pi / length)
    return (jnp.cos(angles), handed * jnp.sin(angles))


def complex_table(length, handed):
    cosine, sine_part = phases(length, length, length, handed)
    return jnp.stack([jnp.stack([cosine, sine_part]), jnp.stack([-sine_part, cosine])])


def depth_tables(length):
    factor = float(length) ** (-1.5)
    cosine, sine_part = phases(length, length // 2, length, 1.0)
    weight = jnp.where(lax.broadcasted_iota(jnp.int32, (length // 2, 1), 0) == 0, 1.0, 2.0)
    backward = jnp.stack([weight * cosine, -weight * sine_part]) * factor
    onward = jnp.stack([cosine.T, -sine_part.T], axis=1) * factor
    return (backward, onward)


def slab_spread(fields, group_size, slab_width, table):
    points = table.shape[-1]
    return jnp.einsum(
        "rmlk,rskgx->gsxlm",
        fields,
        table.reshape(2, 2, points, group_size, slab_width),
        precision=highest,
    )


def slab_rows(received, group_size, cross_part, table, components):
    points = table.shape[-1]
    strips = jnp.einsum(
        "grxlm,rsgly->sxmy",
        received,
        table.reshape(2, 2, group_size, cross_part, points),
        precision=highest,
    )
    return strips.reshape(2, strips.shape[1], components, -1, points)


def slab_planes(physical, group_size, cross_part, onward_cut, table):
    components, slab_width, points = (physical.shape[0], physical.shape[1], physical.shape[3])
    depth_part = onward_cut.shape[2]
    planes = jnp.einsum("cxyz,zrj->rxcjy", physical, onward_cut, precision=highest)
    return jnp.einsum(
        "rxmy,rsygl->gsxlm",
        planes.reshape(2, slab_width, components * depth_part, points),
        table.reshape(2, 2, points, group_size, cross_part),
        precision=highest,
    )


def slab_close(received, group_size, slab_width, table):
    points = table.shape[-1]
    return jnp.einsum(
        "gsxlm,srgxk->rmlk",
        received,
        table.reshape(2, 2, group_size, slab_width, points),
        precision=highest,
    )


def turned(field):
    return jnp.stack([-field[1], field[0]])


def on_device(velocity_hat, time_step, power, cutoffs):
    count_y = lax.axis_size("py")
    count_z = lax.axis_size("pz")
    group_size = count_y * count_z
    half_depth = velocity_hat.shape[2]
    points = 2 * half_depth
    cross_part = velocity_hat.shape[3] // points
    flat_width = velocity_hat.shape[3]
    slab_width = points // group_size
    depth_keep = min(half_depth, (points // 3 + 8) // 8 * 8)
    inverse_table = complex_table(points, 1.0)
    forward_table = complex_table(points, -1.0)
    backward, onward = depth_tables(points)
    backward_cut = backward[:, :depth_keep]
    onward_cut = onward[:, :, :depth_keep]
    depth_wave = lax.broadcasted_iota(jnp.int32, (half_depth, 1, 1), 0)
    cross_index = lax.axis_index(("py", "pz")) * cross_part + lax.broadcasted_iota(
        jnp.int32, (1, cross_part, 1), 1
    )
    cross_wave = jnp.where(cross_index < points // 2, cross_index, cross_index - points)
    along_index = lax.broadcasted_iota(jnp.int32, (1, 1, points), 2)
    along_wave = jnp.where(along_index < points // 2, along_index, along_index - points)
    keep_mask = (
        (jnp.abs(along_wave) <= cutoffs[0])
        & (jnp.abs(cross_wave) <= cutoffs[1])
        & (depth_wave <= cutoffs[2])
    ).astype(jnp.float32)
    waves = (
        along_wave.astype(jnp.float32),
        cross_wave.astype(jnp.float32),
        depth_wave.astype(jnp.float32),
    )
    wave_square = waves[0] * waves[0] + waves[1] * waves[1] + waves[2] * waves[2]
    inverse_square = 1.0 / jnp.maximum(wave_square, 1.0)

    def project(field):
        normal_part = waves[0] * field[:, 0] + waves[1] * field[:, 1] + waves[2] * field[:, 2]
        return jnp.stack(
            [
                keep_mask
                * (field[:, axis_index] - waves[axis_index] * normal_part * inverse_square)
                for axis_index in range(3)
            ],
            axis=1,
        )

    step_size = time_step[0]
    current = velocity_hat.reshape(2, 3, half_depth, cross_part, points)
    solenoidal = project(current)
    kept = solenoidal[:, :, :depth_keep]
    fields = jnp.concatenate(
        [
            kept,
            turned(waves[0] * kept[:, 2])[:, None],
            turned(waves[0] * kept[:, 1] - waves[1] * kept[:, 0])[:, None],
        ],
        axis=1,
    ).reshape(2, 5 * depth_keep, cross_part, points)
    received = lax.all_to_all(
        slab_spread(fields, group_size, slab_width, inverse_table),
        ("py", "pz"),
        split_axis=0,
        concat_axis=0,
        tiled=True,
    )
    row_index = lax.broadcasted_iota(jnp.int32, (points, 1), 0)
    row_wave = jnp.where(row_index < points // 2, row_index, row_index - points)
    row_wave = row_wave.astype(jnp.float32)
    slope_table = jnp.stack(
        [-row_wave * inverse_table[:, 1], row_wave * inverse_table[:, 0]], axis=1
    )
    rows = slab_rows(received, group_size, cross_part, inverse_table, 5)
    slope = slab_rows(
        received[..., 2 * depth_keep : 3 * depth_keep], group_size, cross_part, slope_table, 1
    )
    kz = lax.broadcasted_iota(jnp.int32, (depth_keep, 1), 0).astype(jnp.float32)
    strips = jnp.stack(
        [
            rows[:, :, 0],
            rows[:, :, 1],
            rows[:, :, 2],
            slope[:, :, 0] - turned(kz * rows[:, :, 1]),
            turned(kz * rows[:, :, 0]) - rows[:, :, 3],
            rows[:, :, 4],
        ],
        axis=2,
    )
    physical = jnp.einsum("sxcjy,sjz->cxyz", strips, backward_cut, precision=highest)
    velocity = physical[:3]
    vorticity = physical[3:]
    nonlinear = jnp.stack(
        [
            velocity[1] * vorticity[2] - velocity[2] * vorticity[1],
            velocity[2] * vorticity[0] - velocity[0] * vorticity[2],
            velocity[0] * vorticity[1] - velocity[1] * vorticity[0],
        ]
    )
    local_fastest = jnp.max(jnp.abs(velocity[0]) + jnp.abs(velocity[1]) + jnp.abs(velocity[2]))
    local_squares = jnp.sum(velocity * velocity)
    fastest = lax.pmax(local_fastest, ("py", "pz"))
    summed = lax.psum(local_squares, ("py", "pz"))
    energy = 0.5 * summed / float(points**3)
    layers = slab_planes(nonlinear, group_size, cross_part, onward_cut, forward_table)
    spectra = slab_close(
        lax.all_to_all(layers, ("py", "pz"), split_axis=0, concat_axis=0, tiled=True),
        group_size,
        slab_width,
        forward_table,
    ).reshape(2, 3, depth_keep, cross_part, points)
    spectra = jnp.concatenate(
        [spectra, jnp.zeros((2, 3, half_depth - depth_keep, cross_part, points), jnp.float32)],
        axis=2,
    )
    forced = project(spectra)
    forcing = power[0] / jnp.maximum(2.0 * energy, 0.5)
    update = solenoidal + step_size * (
        forced + forcing * solenoidal - viscosity * wave_square * solenoidal
    )
    keep_weight = keep_share[0]
    current = keep_weight * solenoidal + (1.0 - keep_weight) * update
    cfl_values = [step_size * fastest * points / (2.0 * math.pi)]
    energy_values = [energy]
    velocity_next = current.reshape(2, 3, half_depth, flat_width)
    return (velocity_next, jnp.stack(cfl_values), jnp.stack(energy_values))


def solution(mesh):
    return jax.shard_map(
        on_device,
        mesh=mesh,
        in_specs=(P("member", None, None, ("py", "pz")), P("member"), P("member"), P("member")),
        out_specs=(P("member", None, None, ("py", "pz")), P("member"), P("member")),
        check_vma=False,
    )
```
